32 devices in a mesh: row: 4 (over y, x), col: 4 (over z), depth: 2 (over core).
Axes of the slice: x: 2, y: 2, z: 4, core: 2. Of those that a mesh axis runs over, the one named last changes fastest.
Arguments:
- matrix_columns: float32 [4, 8, 768, 24576], P(None, ('col', 'depth'), None, 'row'), may hold values from -0.0390625 to 0.0390625
- sources: float32 [4, 8, 768, 128], P('row', ('col', 'depth')), may hold values from -6 to 6
Outputs:
- first_image: float32 [4, 8, 768, 128], P('row', ('col', 'depth'))
- second_image: float32 [4, 8, 768, 128], P('row', ('col', 'depth'))
The draws below stay inside these ranges and needn't reach their ends.
All inputs are finite; a program needn't handle non-finite values.
Results may differ from the reference program's by a relative error of at most 0.00011.
Values sent between devices are 32-bit elements; how exact they have to be, the bound alone decides.
A program may use at most 128 MiB of HBM per device.

```python
import jax
import jax.numpy as jnp
from jax import lax

ORDER = 24576
RHS = 128
PIECE = 768
N_ROW = 4
N_COL = 4
N_DEPTH = 2


def levels(key, shape, shards, least, high):
    gain = 1.0
    for position, parts in shards:
        draws = jax.random.uniform(jax.random.fold_in(jax.random.fold_in(key, 6), position), (parts,), jnp.float32, least / len(shards), high / len(shards))
        gain = gain * jnp.repeat(jnp.exp(draws), shape[position] // parts).reshape((-1,) + (1,) * (len(shape) - 1 - position))
    return gain


def noise(key, dims, width, limit, split=(), held_as=jnp.bfloat16):
    result = jax.random.normal(key, dims, jnp.float32) * width
    if len(split) > 0:
        result = levels(key, dims, split, -0.22, 0.18) * result
    return jnp.clip(result, min=-limit, max=limit).astype(held_as)


def setup_inputs(seed: int = 0) -> dict:
    keys = jax.random.split(jax.random.key(seed), 3)
    matrix_columns = noise(keys[0], (N_ROW, N_COL * N_DEPTH, PIECE, ORDER), ORDER ** -0.5, 0.0390625, ((1, 8), (3, 4)), jnp.float32)
    sources = noise(keys[1], (N_ROW, N_COL * N_DEPTH, PIECE, RHS), 1.0, 6.0, ((0, 4), (1, 8)), jnp.float32)
    return {"matrix_columns": matrix_columns, "sources": sources}


def apply_matrix(matrix_t, vectors):
    return lax.dot_general(matrix_t, vectors, (((0,), (0,)), ((), ())), precision=lax.Precision.HIGHEST, preferred_element_type=jnp.float32)


def reference(matrix_columns, sources):
    matrix_t = matrix_columns.reshape(ORDER, ORDER)
    inputs_flat = sources.reshape(ORDER, RHS)
    first_flat = apply_matrix(matrix_t, inputs_flat)
    second_flat = apply_matrix(matrix_t, first_flat)
    return first_flat.reshape(sources.shape), second_flat.reshape(sources.shape)
```

```python
import functools
import math

import jax
import jax.numpy as jnp
from jax import lax
from jax.experimental import pallas as pl
from jax.experimental.pallas import tpu as pltpu
from jax.sharding import PartitionSpec as P

MESH = pl.DeviceIdType.MESH
LANES = 128
VMEM_BYTES = 67043328
VMEM_SPARE = 1 << 20
RING = 2
LAG = 3
PASSES = 2


def split(values):
    high = values.astype(jnp.bfloat16)
    low = (values - high.astype(jnp.float32)).astype(jnp.bfloat16)
    return high, low


class Plan:
    def __init__(self, mesh_shape, columns_shape, width):
        self.n_row = mesh_shape["row"]
        self.n_z = mesh_shape["col"]
        self.n_core = mesh_shape["depth"]
        assert self.n_core == 2
        side = math.isqrt(self.n_row)
        self.n_x = side if side * side == self.n_row else self.n_row
        self.n_y = self.n_row // self.n_x
        self.outer, _, self.piece, self.rows = columns_shape
        self.width = width
        self.fused = self.piece % LANES == 0 and self.n_z % 2 == 0
        self.chunk = LANES if self.fused else self.piece
        self.chunks = self.piece // self.chunk
        if self.fused:
            self.lanes = 4 * self.chunk
        else:
            self.lanes = math.gcd(self.rows, 4 * LANES)
        self.steps = self.rows // self.lanes
        self.pairs = self.n_z * self.chunks // 2
        self.k_depth = math.gcd(self.piece, 2 * LANES)
        self.core_base = 0 if self.fused else self.steps - 1
        self.base = self.core_base + 1
        last = 0
        for z in range(self.n_z):
            last = max(last, (self.n_z - 1 - z) * self.chunks - 1 + self.base + z * LAG)
            last = max(last, self.final_base(z, max) + self.chunks - 1)
        self.iterations = max(last + 1, self.steps, self.core_base + self.pairs)
        self.hops = (self.n_z - 1) * self.chunks
        step_bytes = 4 * self.outer * self.piece * self.lanes
        other = 4 * width * (
            self.rows
            + PASSES * self.n_z * self.chunks * self.chunk
            + 2 * PASSES * self.hops * self.chunk
            + PASSES * self.n_row * self.piece
            + (PASSES + 1) * self.piece
            + self.outer * self.piece
        )
        self.slots = min(self.steps, (VMEM_BYTES - VMEM_SPARE - other) // step_bytes)
        self.resident = self.steps if self.slots == self.steps else self.slots - RING
        self.ringed = self.steps - self.resident
        assert self.ringed == 0 or 0 <= 2 * self.resident <= self.steps

    def final_base(self, z, largest=jnp.maximum):
        right = (self.n_z - 1 - z) * self.chunks + z * LAG
        left = z * self.chunks + (self.n_z - 1 - z) * LAG
        if largest is max:
            if z == 0:
                return self.base + left
            if z == self.n_z - 1:
                return self.base + right
            return self.base + max(left, right)
        right = jnp.where(z > 0, right, 0)
        left = jnp.where(z < self.n_z - 1, left, 0)
        return self.base + largest(left, right)

    def scratch(self):
        f32 = jnp.float32
        chunk = (self.chunk, self.width)
        dma = pltpu.SemaphoreType.DMA
        pieces = self.n_z * self.chunks
        links = max(1, self.n_x + self.n_y - 2)
        relays = max(1, (self.n_x - 1) * (self.n_y - 1))
        parts = 4 if self.fused else 1
        return dict(
            a_buf=pltpu.VMEM((self.slots, self.outer, self.piece, self.lanes), f32),
            xt=pltpu.VMEM((self.outer, 2 * self.width, self.piece), jnp.bfloat16),
            acc=pltpu.VMEM((self.rows, self.width), f32),
            core_rx=pltpu.VMEM((PASSES, pieces) + chunk, f32),
            left_rx=pltpu.VMEM((PASSES, self.hops) + chunk, f32),
            right_rx=pltpu.VMEM((PASSES, self.hops) + chunk, f32),
            xg=pltpu.VMEM((PASSES, self.n_row, self.chunks) + chunk, f32),
            own=pltpu.VMEM((PASSES + 1, self.chunks) + chunk, f32),
            a_sem=dma((self.slots, parts)),
            io_sem=dma((3,)),
            ag_send=dma((PASSES, self.chunks, links)),
            ag_recv=dma((PASSES, self.n_row, self.chunks)),
            relay_send=dma((PASSES, self.chunks, relays)),
            core_send=dma((pieces,)),
            core_recv=dma((PASSES, pieces)),
            z_send=dma((pieces,)),
            left_recv=dma((PASSES, self.hops)),
            right_recv=dma((PASSES, self.hops)),
        )


def chain_kernel(
    plan, columns, source, first, second, *, a_buf, xt, acc, core_rx, left_rx, right_rx, xg, own,
    a_sem, io_sem, ag_send, ag_recv, relay_send, core_send, core_recv, z_send, left_recv, right_recv,
):
    n_z, n_x, n_y = plan.n_z, plan.n_x, plan.n_y
    chunk, chunks, width, piece = plan.chunk, plan.chunks, plan.width, plan.piece
    row, z, core = lax.axis_index("row"), lax.axis_index("col"), lax.axis_index("depth")
    x, y = lax.rem(row, n_x), lax.div(row, n_x)

    x_rows = [y * n_x + lax.rem(x + i, n_x) for i in range(1, n_x)]
    y_rows = [lax.rem(y + i, n_y) * n_x + x for i in range(1, n_y)]
    diagonal = [
        lax.rem(y + i, n_y) * n_x + lax.rem(x + k, n_x) for i in range(1, n_y) for k in range(1, n_x)
    ]
    left, right = (row, z - 1, core), (row, z + 1, core)
    partner = (row, z, 1 - core)

    def piece_chunks(pair):
        at, j = lax.div(pair, chunks), lax.rem(pair, chunks)
        return (n_z - 1 - at, j), (at, j)

    def row_start(at, on_core, j):
        return pl.multiple_of((at * 2 + on_core) * piece + j * chunk, 8 if not plan.fused else LANES)

    def loads(k, slot):
        if not plan.fused:
            lanes = pl.ds(pl.multiple_of(k * plan.lanes, LANES), plan.lanes)
            return [pltpu.make_async_copy(columns.at[:, 0, :, lanes], a_buf.at[slot], a_sem.at[slot, 0])]
        result = []
        for at, j in piece_chunks(k):
            for on_core in range(2):
                i = len(result)
                result.append(
                    pltpu.make_async_copy(
                        columns.at[:, 0, :, pl.ds(row_start(at, on_core, j), chunk)],
                        a_buf.at[slot, :, :, i * chunk:(i + 1) * chunk],
                        a_sem.at[slot, i],
                    )
                )
        return result

    def load(k, slot):
        for copy in loads(k, slot):
            copy.start()

    def ring_step(i):
        i = lax.rem(i, plan.ringed)
        return jnp.where(i <= plan.resident, 2 * i, plan.resident + i)

    def ring_slot(i):
        return plan.resident + lax.rem(i, RING)

    own_in = pltpu.make_async_copy(source, own.at[0], io_sem.at[0])
    own_in.start()
    if plan.ringed == 0:
        for k in range(plan.steps):
            load(k, k)
    else:
        for k in range(max(2 * plan.resident, 2 * RING)):
            if k % 2 == 1 and k < 2 * plan.resident:
                load(k, k // 2)
            if k % 2 == 0 and k < 2 * RING:
                load(ring_step(k // 2), ring_slot(k // 2))

    barrier = pltpu.get_barrier_semaphore()
    for other in x_rows + y_rows:
        pl.semaphore_signal(barrier, inc=1, device_id=(other, z, core), device_id_type=MESH)
    pl.semaphore_signal(barrier, inc=1, device_id=partner, device_id_type=MESH)

    @pl.when(z > 0)
    def _():
        pl.semaphore_signal(barrier, inc=1, device_id=left, device_id_type=MESH)

    @pl.when(z < n_z - 1)
    def _():
        pl.semaphore_signal(barrier, inc=1, device_id=right, device_id_type=MESH)

    beside = jnp.where(z > 0, 1, 0) + jnp.where(z < n_z - 1, 1, 0)
    pl.semaphore_wait(barrier, n_x + n_y - 1 + beside)

    own_in.wait()

    def spread(p, j, i, other):
        return pltpu.make_async_remote_copy(
            src_ref=own.at[p, j], dst_ref=xg.at[p, row, j],
            send_sem=ag_send.at[p, j, i], recv_sem=ag_recv.at[p, row, j],
            device_id=(other, z, core), device_id_type=MESH,
        )

    def relay(p, j, i, origin, other):
        return pltpu.make_async_remote_copy(
            src_ref=xg.at[p, origin, j], dst_ref=xg.at[p, origin, j],
            send_sem=relay_send.at[p, j, i], recv_sem=ag_recv.at[p, origin, j],
            device_id=(other, z, core), device_id_type=MESH,
        )

    def spread_all(p, j):
        for i, other in enumerate(x_rows + y_rows):
            spread(p, j, i, other).start()

    def place(origin, j, ref):
        high, low = split(ref[...].T)
        xt[origin, :width, j * chunk:(j + 1) * chunk] = high
        xt[origin, width:, j * chunk:(j + 1) * chunk] = low

    def gather(p):
        for j in range(chunks):
            place(row, j, own.at[p, j])
            near, far = (x_rows, y_rows) if j % 2 == 0 else (y_rows, x_rows)
            for i, origin in enumerate(near):
                relay(p, j, 0, origin, row).wait_recv()
                for k, other in enumerate(far):
                    relay(p, j, i * len(far) + k, origin, other).start()
                place(origin, j, xg.at[p, origin, j])
            for origin in far:
                relay(p, j, 0, origin, row).wait_recv()
                place(origin, j, xg.at[p, origin, j])
        for j in range(chunks):
            for origin in diagonal:
                relay(p, j, 0, origin, row).wait_recv()
                place(origin, j, xg.at[p, origin, j])

    def to_core(p, at, j):
        return pltpu.make_async_remote_copy(
            src_ref=acc.at[pl.ds(row_start(at, 1 - core, j), chunk), :],
            dst_ref=core_rx.at[p, at * chunks + j],
            send_sem=core_send.at[at * chunks + j], recv_sem=core_recv.at[p, at * chunks + j],
            device_id=partner, device_id_type=MESH,
        )

    def to_right(p, at, j):
        q = (n_z - 1 - at) * chunks + j
        return pltpu.make_async_remote_copy(
            src_ref=acc.at[pl.ds(row_start(at, core, j), chunk), :],
            dst_ref=left_rx.at[p, q],
            send_sem=z_send.at[at * chunks + j], recv_sem=left_recv.at[p, q],
            device_id=right, device_id_type=MESH,
        )

    def to_left(p, at, j):
        q = at * chunks + j
        return pltpu.make_async_remote_copy(
            src_ref=acc.at[pl.ds(row_start(at, core, j), chunk), :],
            dst_ref=right_rx.at[p, q],
            send_sem=z_send.at[at * chunks + j], recv_sem=right_recv.at[p, q],
            device_id=left, device_id_type=MESH,
        )

    def sent(p, at, j):
        to_core(p, at, j).wait_send()

        @pl.when(at > z)
        def _():
            to_right(p, at, j).wait_send()

        @pl.when(at < z)
        def _():
            to_left(p, at, j).wait_send()

    def multiply(p, k):
        if plan.ringed == 0:
            held, slot = True, k
        else:
            held = jnp.logical_and(lax.rem(k, 2) == 1, k < 2 * plan.resident)
            ring_at = p * plan.ringed + jnp.where(k < 2 * plan.resident, lax.div(k, 2), k - plan.resident)
            slot = jnp.where(held, lax.div(k, 2), ring_slot(ring_at))

        @pl.when(jnp.logical_or(p == 0, jnp.logical_not(held)))
        def _():
            for copy in loads(k, slot):
                copy.wait()

        main = rest = None
        for a in range(plan.outer):
            for at in range(0, piece, plan.k_depth):
                span = slice(at, at + plan.k_depth)
                high, low = split(a_buf[slot, a, span, :])
                both = jnp.dot(xt[a, :, span], high, preferred_element_type=jnp.float32)
                side = jnp.dot(xt[a, :width, span], low, preferred_element_type=jnp.float32)
                main = both if main is None else main + both
                rest = side if rest is None else rest + side
        total = (main[:width] + (main[width:] + rest)).T
        if plan.fused:
            i = 0
            for at, j in piece_chunks(k):
                for on_core in range(2):
                    acc[pl.ds(row_start(at, on_core, j), chunk), :] = total[i * chunk:(i + 1) * chunk]
                    i += 1
        else:
            acc[pl.ds(pl.multiple_of(k * plan.lanes, LANES), plan.lanes), :] = total

        if plan.ringed > 0:
            follow = ring_at + RING

            @pl.when(jnp.logical_and(jnp.logical_not(held), follow < PASSES * plan.ringed))
            def _():
                load(ring_step(follow), ring_slot(follow))

    def own_sum(p, at, j):
        to_core(p, at, j).wait_recv()
        mine = pl.ds(row_start(at, core, j), chunk)
        acc[mine, :] = acc[mine, :] + core_rx[p, at * chunks + j]
        return mine

    def iteration(k, p):
        @pl.when(k < plan.steps)
        def _():
            @pl.when(p > 0)
            def _():
                if plan.fused:
                    for at, j in piece_chunks(k):
                        sent(p, at, j)
                else:
                    @pl.when(k == 0)
                    def _():
                        sent_all(p)
            multiply(p, k)

        pair = k - plan.core_base

        @pl.when(jnp.logical_and(pair >= 0, pair < plan.pairs))
        def _():
            for at, j in piece_chunks(pair):
                to_core(p, at, j).start()

        q = k - plan.base - z * LAG

        @pl.when(jnp.logical_and(q >= 0, q < (n_z - 1 - z) * chunks))
        def _():
            at, j = n_z - 1 - lax.div(q, chunks), lax.rem(q, chunks)
            mine = own_sum(p, at, j)

            @pl.when(z > 0)
            def _():
                to_right(p, at, j).wait_recv()
                acc[mine, :] = acc[mine, :] + left_rx[p, q]

            to_right(p, at, j).start()

        s = k - plan.base - (n_z - 1 - z) * LAG

        @pl.when(jnp.logical_and(s >= 0, s < z * chunks))
        def _():
            at, j = lax.div(s, chunks), lax.rem(s, chunks)
            mine = own_sum(p, at, j)

            @pl.when(z < n_z - 1)
            def _():
                to_left(p, at, j).wait_recv()
                acc[mine, :] = acc[mine, :] + right_rx[p, s]

            to_left(p, at, j).start()

        f = k - plan.final_base(z)

        @pl.when(jnp.logical_and(f >= 0, f < chunks))
        def _():
            mine = own_sum(p, z, f)

            @pl.when(z > 0)
            def _():
                to_right(p, z, f).wait_recv()
                acc[mine, :] = acc[mine, :] + left_rx[p, (n_z - 1 - z) * chunks + f]

            @pl.when(z < n_z - 1)
            def _():
                to_left(p, z, f).wait_recv()
                acc[mine, :] = acc[mine, :] + right_rx[p, z * chunks + f]

            own[p + 1, f] = acc[mine, :]

            @pl.when(p + 1 < PASSES)
            def _():
                spread_all(p + 1, f)

        return p

    def sent_all(p):
        def one(i, carry):
            sent(p, lax.div(i, chunks), lax.rem(i, chunks))
            return carry

        lax.fori_loop(0, n_z * chunks, one, 0)

    out_first = pltpu.make_async_copy(own.at[1], first, io_sem.at[1])
    out_second = pltpu.make_async_copy(own.at[2], second, io_sem.at[2])

    for j in range(chunks):
        spread_all(0, j)

    def one_pass(p, carry):
        gather(p)
        lax.fori_loop(0, plan.iterations, iteration, p)

        @pl.when(p == 0)
        def _():
            out_first.start()

        return carry

    lax.fori_loop(0, PASSES, one_pass, 0)
    out_second.start()
    sent_all(PASSES - 1)
    for p in range(PASSES):
        for j in range(chunks):
            for i, other in enumerate(x_rows + y_rows):
                spread(p, j, i, other).wait_send()
            for i in range((n_x - 1) * (n_y - 1)):
                relay(p, j, i, row, row).wait_send()
    out_first.wait()
    out_second.wait()


def solution(mesh):
    def body(matrix_columns, sources):
        plan = Plan(dict(mesh.shape), matrix_columns.shape, sources.shape[-1])
        blocked = (plan.chunks, plan.chunk, plan.width)
        image = jax.ShapeDtypeStruct(blocked, jnp.float32)
        anywhere = pl.BlockSpec(memory_space=pl.ANY)
        scratch = plan.scratch()
        products = PASSES * plan.rows * plan.outer * plan.piece
        first, second = pl.pallas_call(
            functools.partial(chain_kernel, plan),
            out_shape=(image, image),
            in_specs=[anywhere, anywhere],
            out_specs=(anywhere, anywhere),
            scratch_shapes=scratch,
            compiler_params=pltpu.CompilerParams(
                collective_id=0, has_side_effects=True, vmem_limit_bytes=VMEM_BYTES
            ),
            cost_estimate=pl.CostEstimate(
                flops=6 * products * plan.width, bytes_accessed=4 * products, transcendentals=0
            ),
        )(matrix_columns, sources.reshape(blocked))
        return first.reshape(sources.shape), second.reshape(sources.shape)

    in_specs = (P(None, ("col", "depth"), None, "row"), P("row", ("col", "depth"), None, None))
    out_specs = (P("row", ("col", "depth"), None, None), P("row", ("col", "depth"), None, None))
    return jax.shard_map(body, mesh=mesh, in_specs=in_specs, out_specs=out_specs, check_vma=False)
```

```python
import functools
import math

import jax
import jax.numpy as jnp
from jax import lax
from jax.experimental import pallas as pl
from jax.experimental.pallas import tpu as pltpu
from jax.sharding import PartitionSpec as P

MESH = pl.DeviceIdType.MESH
LANES = 128
VMEM_BYTES = 67043328
VMEM_SPARE = 256 << 10
RING = 2
LAG = 3
RELAY = 2
PASSES = 2


def split(values):
    high = values.astype(jnp.bfloat16)
    low = (values - high.astype(jnp.float32)).astype(jnp.bfloat16)
    return high, low


class Plan:
    def __init__(self, mesh_shape, columns_shape, width):
        self.n_row = mesh_shape["row"]
        self.n_z = mesh_shape["col"]
        assert mesh_shape["depth"] == 2
        side = math.isqrt(self.n_row)
        self.n_x = side if side * side == self.n_row else self.n_row
        self.n_y = self.n_row // self.n_x
        self.outer, _, self.piece, self.rows = columns_shape
        self.width = width
        self.fused = self.piece % LANES == 0 and self.n_z % 2 == 0 and self.n_z >= 4
        self.chunk = LANES if self.fused else self.piece
        self.chunks = self.piece // self.chunk
        self.per_step = 4 if self.fused else math.lcm(self.piece, LANES) // self.piece
        self.lanes = self.per_step * self.chunk
        self.steps = self.rows // self.lanes
        self.ids = self.n_z * self.chunks
        self.k_depth = math.gcd(self.piece, 2 * LANES)
        self.base = 1 if self.fused else self.steps
        finals = max(self.final_start(z) for z in range(self.n_z)) + self.chunks
        self.period = max(self.steps, finals + RELAY)
        self.arrivals = (self.n_z + 1) * self.chunks
        step_bytes = 4 * self.outer * self.piece * self.lanes
        lanes_padded = -(-self.chunk // LANES) * LANES
        other = 4 * self.width * lanes_padded * (
            4 * self.ids
            + PASSES * self.ids
            + PASSES * self.arrivals
            + PASSES * self.n_row * self.chunks
            + (PASSES + 1) * self.chunks
        ) + 4 * self.width * self.outer * self.piece + 8 * self.piece * width
        self.slots = min(self.steps, (VMEM_BYTES - VMEM_SPARE - other) // step_bytes)
        self.resident = self.steps if self.slots == self.steps else self.slots - RING
        self.ringed = self.steps - self.resident
        assert self.ringed == 0 or 0 <= 2 * self.resident <= self.steps

    def final_start(self, z):
        n_z, n = self.n_z, self.chunks
        from_left = (n_z - 1 - z) * n + (0 if self.fused and z == 1 else z * LAG)
        from_right = z * n + (0 if self.fused and z == n_z - 2 else (n_z - 1 - z) * LAG)
        if z == 0:
            from_left = 0
        if z == n_z - 1:
            from_right = 0
        return self.base + max(from_left, from_right)

    def scratch(self):
        f32 = jnp.float32
        chunk = (self.width, self.chunk)
        dma = pltpu.SemaphoreType.DMA
        links = max(1, self.n_x + self.n_y - 2)
        relays = max(1, (self.n_x - 1) * (self.n_y - 1))
        parts = 4 if self.fused else 1
        return dict(
            a_buf=pltpu.VMEM((self.slots, self.outer, self.piece, self.lanes), f32),
            xt=pltpu.VMEM((self.outer, 2 * self.width, self.piece), jnp.bfloat16),
            acc=pltpu.VMEM((PASSES, 2 * self.ids) + chunk, f32),
            core_rx=pltpu.VMEM((PASSES, self.ids) + chunk, f32),
            z_rx=pltpu.VMEM((PASSES, self.arrivals) + chunk, f32),
            xg=pltpu.VMEM((PASSES, self.n_row, self.chunks) + chunk, f32),
            own=pltpu.VMEM((PASSES + 1, self.chunks) + chunk, f32),
            edge=pltpu.VMEM((2, self.chunks, self.chunk, self.width), f32),
            a_sem=dma((self.slots, parts)),
            in_sem=dma(()),
            out_sem=dma((2, self.chunks)),
            ag_send=dma((PASSES, self.chunks, links)),
            ag_recv=dma((PASSES, self.n_row, self.chunks)),
            relay_send=dma((PASSES, self.chunks, relays)),
            core_send=dma((PASSES, self.ids)),
            core_recv=dma((PASSES, self.ids)),
            z_send=dma((PASSES, self.ids)),
            z_recv=dma((PASSES, self.arrivals)),
        )


def chain_kernel(
    plan, columns, source, first, second, *, a_buf, xt, acc, core_rx, z_rx, xg, own, edge,
    a_sem, in_sem, out_sem, ag_send, ag_recv, relay_send, core_send, core_recv, z_send, z_recv,
):
    n_z, n_x, n_y = plan.n_z, plan.n_x, plan.n_y
    chunk, chunks, width, piece = plan.chunk, plan.chunks, plan.width, plan.piece
    steps = plan.steps
    row, z, core = lax.axis_index("row"), lax.axis_index("col"), lax.axis_index("depth")
    x, y = lax.rem(row, n_x), lax.div(row, n_x)
    at_left, at_right = z == 0, z == n_z - 1

    x_rows = [y * n_x + lax.rem(x + i, n_x) for i in range(1, n_x)]
    y_rows = [lax.rem(y + i, n_y) * n_x + x for i in range(1, n_y)]
    diagonal = [
        lax.rem(y + i, n_y) * n_x + lax.rem(x + k, n_x) for i in range(1, n_y) for k in range(1, n_x)
    ]
    left, right = (row, z - 1, core), (row, z + 1, core)
    partner = (row, z, 1 - core)

    def piece_of(at):
        return sum(jnp.where(at >= n * chunks, 1, 0) for n in range(1, n_z))

    def rightward(q):
        return q + (n_z - 1 - 2 * piece_of(q)) * chunks

    def place_of(at, on_core):
        return at + (piece_of(at) + on_core) * chunks

    def step_ids(k):
        one = jnp.where(at_left, rightward(2 * k), jnp.where(at_right, 2 * k, rightward(k)))
        two = jnp.where(at_left, rightward(2 * k + 1), jnp.where(at_right, 2 * k + 1, k))
        return one, two

    def loads(k, slot):
        if not plan.fused:
            lanes = pl.ds(pl.multiple_of(k * plan.lanes, LANES), plan.lanes)
            return [pltpu.make_async_copy(columns.at[:, 0, :, lanes], a_buf.at[slot], a_sem.at[slot, 0])]
        result = []
        for at in step_ids(k):
            for on_core in range(2):
                i = len(result)
                lanes = pl.ds(pl.multiple_of(place_of(at, on_core) * chunk, LANES), chunk)
                result.append(
                    pltpu.make_async_copy(
                        columns.at[:, 0, :, lanes],
                        a_buf.at[slot, :, :, i * chunk:(i + 1) * chunk],
                        a_sem.at[slot, i],
                    )
                )
        return result

    def load(k, slot):
        for copy in loads(k, slot):
            copy.start(priority=1)

    def ring_step(i):
        i = jnp.where(i >= plan.ringed, i - plan.ringed, i)
        return jnp.where(i <= plan.resident, 2 * i, plan.resident + i)

    def ring_slot(i):
        return plan.resident + lax.rem(i, RING)

    source_in = pltpu.make_async_copy(source, edge.at[0], in_sem)
    source_in.start()
    if plan.ringed == 0:
        for k in range(steps):
            load(k, k)
    else:
        for k in range(max(2 * plan.resident, 2 * RING)):
            if k % 2 == 1 and k < 2 * plan.resident:
                load(k, k // 2)
            if k % 2 == 0 and k < 2 * RING:
                load(ring_step(k // 2), ring_slot(k // 2))

    barrier = pltpu.get_barrier_semaphore()
    for other in x_rows + y_rows:
        pl.semaphore_signal(barrier, inc=1, device_id=(other, z, core), device_id_type=MESH)
    pl.semaphore_signal(barrier, inc=1, device_id=partner, device_id_type=MESH)

    @pl.when(jnp.logical_not(at_left))
    def _():
        pl.semaphore_signal(barrier, inc=1, device_id=left, device_id_type=MESH)

    @pl.when(jnp.logical_not(at_right))
    def _():
        pl.semaphore_signal(barrier, inc=1, device_id=right, device_id_type=MESH)

    beside = jnp.where(at_left, 0, 1) + jnp.where(at_right, 0, 1)

    source_in.wait()
    for j in range(chunks):
        own[0, j] = edge[0, j].T

    pl.semaphore_wait(barrier, n_x + n_y - 1 + beside)

    def spread(p, j, i, other):
        return pltpu.make_async_remote_copy(
            src_ref=own.at[p, j], dst_ref=xg.at[p, row, j],
            send_sem=ag_send.at[p, j, i], recv_sem=ag_recv.at[p, row, j],
            device_id=(other, z, core), device_id_type=MESH,
        )

    def relay(p, j, i, origin, other):
        return pltpu.make_async_remote_copy(
            src_ref=xg.at[p, origin, j], dst_ref=xg.at[p, origin, j],
            send_sem=relay_send.at[p, j, i], recv_sem=ag_recv.at[p, origin, j],
            device_id=(other, z, core), device_id_type=MESH,
        )

    def spread_all(p, j):
        for i, other in enumerate(x_rows + y_rows):
            spread(p, j, i, other).start()

    def pass_on(p, j, near, far):
        for i, origin in enumerate(near):
            relay(p, j, 0, origin, row).wait_recv()
            for k, other in enumerate(far):
                relay(p, j, i * len(far) + k, origin, other).start()

    def place(origin, j, ref):
        high, low = split(ref[...])
        xt[origin, :width, j * chunk:(j + 1) * chunk] = high
        xt[origin, width:, j * chunk:(j + 1) * chunk] = low

    def sides(j):
        return (x_rows, y_rows) if j % 2 == 0 else (y_rows, x_rows)

    def gather(p):
        @pl.when(p == 0)
        def _():
            for j in range(chunks):
                pass_on(p, j, *sides(j))

        for j in range(chunks):
            near, far = sides(j)
            place(row, j, own.at[p, j])
            for origin in near:
                place(origin, j, xg.at[p, origin, j])
            for origin in far:
                relay(p, j, 0, origin, row).wait_recv()
                place(origin, j, xg.at[p, origin, j])
        for j in range(chunks):
            for origin in diagonal:
                relay(p, j, 0, origin, row).wait_recv()
                place(origin, j, xg.at[p, origin, j])

    def to_core(p, at):
        return pltpu.make_async_remote_copy(
            src_ref=acc.at[p, place_of(at, 1 - core)],
            dst_ref=core_rx.at[p, at],
            send_sem=core_send.at[p, at], recv_sem=core_recv.at[p, at],
            device_id=partner, device_id_type=MESH,
        )

    def along(p, at, slot, other):
        return pltpu.make_async_remote_copy(
            src_ref=acc.at[p, place_of(at, core)],
            dst_ref=z_rx.at[p, slot],
            send_sem=z_send.at[p, at], recv_sem=z_recv.at[p, slot],
            device_id=other, device_id_type=MESH,
        )

    def to_right(p, q):
        return along(p, rightward(q), q, right)

    def to_left(p, q):
        return along(p, q, plan.arrivals - 1 - q, left)

    def sent(p, at):
        to_core(p, at).wait_send()

        @pl.when(piece_of(at) != z)
        def _():
            along(p, at, 0, right).wait_send()

    def sent_all(p):
        def one(at, carry):
            sent(p, at)
            return carry

        lax.fori_loop(0, plan.ids, one, 0)

    def multiply(p, k):
        if plan.ringed == 0:
            held, slot = True, k
        else:
            held = jnp.logical_and(lax.rem(k, 2) == 1, k < 2 * plan.resident)
            ring_at = p * plan.ringed + jnp.where(k < 2 * plan.resident, lax.div(k, 2), k - plan.resident)
            slot = jnp.where(held, lax.div(k, 2), ring_slot(ring_at))

        @pl.when(jnp.logical_or(p == 0, jnp.logical_not(held)))
        def _():
            for copy in loads(k, slot):
                copy.wait()

        main = rest = None
        for a in range(plan.outer):
            for at in range(0, piece, plan.k_depth):
                span = slice(at, at + plan.k_depth)
                high, low = split(a_buf[slot, a, span, :])
                both = jnp.dot(xt[a, :, span], high, preferred_element_type=jnp.float32)
                side = jnp.dot(xt[a, :width, span], low, preferred_element_type=jnp.float32)
                main = both if main is None else main + both
                rest = side if rest is None else rest + side
        total = main[:width] + (main[width:] + rest)
        if plan.fused:
            at = [place_of(at, on_core) for at in step_ids(k) for on_core in range(2)]
        else:
            at = [k * plan.per_step + i for i in range(plan.per_step)]
        for i, where in enumerate(at):
            acc[p, where] = total[:, i * chunk:(i + 1) * chunk]

        if plan.ringed > 0:
            follow = ring_at + RING

            @pl.when(jnp.logical_and(jnp.logical_not(held), follow < PASSES * plan.ringed))
            def _():
                load(ring_step(follow), ring_slot(follow))

    def own_sum(p, at):
        to_core(p, at).wait_recv()
        mine = place_of(at, core)
        acc[p, mine] = acc[p, mine] + core_rx[p, at]
        return mine

    def add_from_left(p, q, mine):
        to_right(p, q).wait_recv()
        acc[p, mine] = acc[p, mine] + z_rx[p, q]

    def add_from_right(p, q, mine):
        to_left(p, q).wait_recv()
        acc[p, mine] = acc[p, mine] + z_rx[p, plan.arrivals - 1 - q]

    def finish(p, f):
        mine = own_sum(p, z * chunks + f)

        @pl.when(jnp.logical_not(at_left))
        def _():
            add_from_left(p, (n_z - 1 - z) * chunks + f, mine)

        @pl.when(jnp.logical_not(at_right))
        def _():
            add_from_right(p, z * chunks + f, mine)

        image = acc[p, mine]
        own[p + 1, f] = image
        edge[p, f] = image.T

        @pl.when(p == 0)
        def _():
            spread_all(1, f)
            pltpu.make_async_copy(edge.at[0, f], first.at[f], out_sem.at[0, f]).start()

        @pl.when(p == 1)
        def _():
            pltpu.make_async_copy(edge.at[1, f], second.at[f], out_sem.at[1, f]).start()

    first_final = sum(jnp.where(z == at, plan.final_start(at), 0) for at in range(n_z))

    def iteration(i, p):
        k = i

        @pl.when(k < steps)
        def _():
            multiply(p, k)

            if plan.fused:
                for at in step_ids(k):
                    to_core(p, at).start()
            else:
                @pl.when(k == steps - 1)
                def _():
                    def one(at, inner):
                        to_core(p, at).start()
                        return inner

                    lax.fori_loop(0, plan.ids, one, 0)

        w = i - plan.base - z * LAG
        for u in range(2 if plan.fused else 1):
            q = jnp.where(at_left, 2 * w + u, w) if plan.fused else w
            also = jnp.logical_or(u == 0, at_left)
            inside = jnp.logical_and(w >= 0, q < (n_z - 1 - z) * chunks)

            @pl.when(jnp.logical_and(also, inside))
            def _(q=q):
                mine = own_sum(p, rightward(q))

                @pl.when(jnp.logical_not(at_left))
                def _():
                    add_from_left(p, q, mine)

                to_right(p, q).start()

        w = i - plan.base - (n_z - 1 - z) * LAG
        for u in range(2 if plan.fused else 1):
            q = jnp.where(at_right, 2 * w + u, w) if plan.fused else w
            also = jnp.logical_or(u == 0, at_right)
            inside = jnp.logical_and(w >= 0, q < z * chunks)

            @pl.when(jnp.logical_and(also, inside))
            def _(q=q):
                mine = own_sum(p, q)

                @pl.when(jnp.logical_not(at_right))
                def _():
                    add_from_right(p, q, mine)

                to_left(p, q).start()

        f = i - first_final

        @pl.when(jnp.logical_and(f >= 0, f < chunks))
        def _():
            finish(p, f)

        j = f - RELAY
        due = jnp.logical_and(p + 1 < PASSES, jnp.logical_and(j >= 0, j < chunks))
        for parity in range(2):
            @pl.when(jnp.logical_and(due, lax.rem(j, 2) == parity))
            def _(parity=parity):
                pass_on(p + 1, j, *sides(parity))

        return p

    for j in range(chunks):
        spread_all(0, j)

    def one_pass(p, carry):
        gather(p)
        lax.fori_loop(0, plan.period, iteration, p)
        return carry

    lax.fori_loop(0, PASSES, one_pass, 0)

    sent_all(0)
    sent_all(1)
    for p in range(PASSES):
        for j in range(chunks):
            for i, other in enumerate(x_rows + y_rows):
                spread(p, j, i, other).wait_send()
            for i in range((n_x - 1) * (n_y - 1)):
                relay(p, j, i, row, row).wait_send()
    for j in range(chunks):
        pltpu.make_async_copy(edge.at[0, j], first.at[j], out_sem.at[0, j]).wait()
        pltpu.make_async_copy(edge.at[1, j], second.at[j], out_sem.at[1, j]).wait()


def solution(mesh):
    def body(matrix_columns, sources):
        plan = Plan(dict(mesh.shape), matrix_columns.shape, sources.shape[-1])
        blocked = (plan.chunks, plan.chunk, plan.width)
        image = jax.ShapeDtypeStruct(blocked, jnp.float32)
        anywhere = pl.BlockSpec(memory_space=pl.ANY)
        products = 2 * plan.rows * plan.outer * plan.piece
        first, second = pl.pallas_call(
            functools.partial(chain_kernel, plan),
            out_shape=(image, image),
            in_specs=[anywhere, anywhere],
            out_specs=(anywhere, anywhere),
            scratch_shapes=plan.scratch(),
            compiler_params=pltpu.CompilerParams(
                collective_id=0, has_side_effects=True, vmem_limit_bytes=VMEM_BYTES
            ),
            cost_estimate=pl.CostEstimate(
                flops=6 * products * plan.width, bytes_accessed=4 * products, transcendentals=0
            ),
        )(matrix_columns, sources.reshape(blocked))
        return first.reshape(sources.shape), second.reshape(sources.shape)

    in_specs = (P(None, ("col", "depth"), None, "row"), P("row", ("col", "depth"), None, None))
    out_specs = (P("row", ("col", "depth"), None, None), P("row", ("col", "depth"), None, None))
    return jax.shard_map(body, mesh=mesh, in_specs=in_specs, out_specs=out_specs, check_vma=False)
```

```python
import functools
import math

import jax
import jax.numpy as jnp
from jax import lax
from jax.experimental import pallas as pl
from jax.experimental.pallas import tpu as pltpu
from jax.sharding import PartitionSpec as P

MESH = pl.DeviceIdType.MESH
LANES = 128
VMEM_BYTES = 67043328
VMEM_SPARE = 256 << 10
RING = 2
LAG = 3
RELAY = 2
PASSES = 2


def split(values):
    high = values.astype(jnp.bfloat16)
    low = (values - high.astype(jnp.float32)).astype(jnp.bfloat16)
    return high, low


class Plan:
    def __init__(self, mesh_shape, columns_shape, width):
        self.n_row = mesh_shape["row"]
        self.n_z = mesh_shape["col"]
        assert mesh_shape["depth"] == 2
        side = math.isqrt(self.n_row)
        self.n_x = side if side * side == self.n_row else self.n_row
        self.n_y = self.n_row // self.n_x
        self.outer, _, self.piece, self.rows = columns_shape
        self.width = width
        self.fused = self.piece % LANES == 0 and self.n_z % 2 == 0 and self.n_z >= 4
        self.chunk = LANES if self.fused else self.piece
        self.chunks = self.piece // self.chunk
        self.per_step = 4 if self.fused else math.lcm(self.piece, LANES) // self.piece
        self.lanes = self.per_step * self.chunk
        self.steps = self.rows // self.lanes
        self.ids = self.n_z * self.chunks
        self.k_depth = math.gcd(self.piece, 2 * LANES)
        self.base = 1 if self.fused else self.steps
        finals = max(self.final_start(z) for z in range(self.n_z)) + self.chunks
        self.period = max(self.steps, finals + RELAY)
        self.arrivals = (self.n_z + 1) * self.chunks
        step_bytes = 4 * self.outer * self.piece * self.lanes
        lanes_padded = -(-self.chunk // LANES) * LANES
        other = 4 * self.width * lanes_padded * (
            4 * self.ids
            + PASSES * self.ids
            + PASSES * self.arrivals
            + PASSES * self.n_row * self.chunks
            + (PASSES + 1) * self.chunks
        ) + 4 * self.width * self.outer * self.piece + 8 * self.piece * width
        self.slots = min(self.steps, (VMEM_BYTES - VMEM_SPARE - other) // step_bytes)
        self.resident = self.steps if self.slots == self.steps else self.slots - RING
        self.ringed = self.steps - self.resident
        assert self.ringed == 0 or 0 <= 2 * self.resident <= self.steps

    def final_start(self, z):
        n_z, n = self.n_z, self.chunks
        from_left = (n_z - 1 - z) * n + (0 if self.fused and z == 1 else z * LAG)
        from_right = z * n + (0 if self.fused and z == n_z - 2 else (n_z - 1 - z) * LAG)
        if z == 0:
            from_left = 0
        if z == n_z - 1:
            from_right = 0
        return self.base + max(from_left, from_right)

    def scratch(self):
        f32 = jnp.float32
        chunk = (self.width, self.chunk)
        dma = pltpu.SemaphoreType.DMA
        links = max(1, self.n_x + self.n_y - 2)
        relays = max(1, (self.n_x - 1) * (self.n_y - 1))
        parts = 4 if self.fused else 1
        return dict(
            a_buf=pltpu.VMEM((self.slots, self.outer, self.piece, self.lanes), f32),
            xt=pltpu.VMEM((self.outer, 2 * self.width, self.piece), jnp.bfloat16),
            acc=pltpu.VMEM((PASSES, 2 * self.ids) + chunk, f32),
            core_rx=pltpu.VMEM((PASSES, self.ids) + chunk, f32),
            z_rx=pltpu.VMEM((PASSES, self.arrivals) + chunk, f32),
            xg=pltpu.VMEM((PASSES, self.n_row, self.chunks) + chunk, f32),
            own=pltpu.VMEM((PASSES + 1, self.chunks) + chunk, f32),
            edge=pltpu.VMEM((2, self.chunks, self.chunk, self.width), f32),
            a_sem=dma((self.slots, parts)),
            in_sem=dma(()),
            out_sem=dma((2, self.chunks)),
            ag_send=dma((PASSES, self.chunks, links)),
            ag_recv=dma((PASSES, self.n_row, self.chunks)),
            relay_send=dma((PASSES, self.chunks, relays)),
            core_send=dma((PASSES, self.ids)),
            core_recv=dma((PASSES, self.ids)),
            z_send=dma((PASSES, self.ids)),
            z_recv=dma((PASSES, self.arrivals)),
        )


def chain_kernel(
    plan, columns, source, first, second, *, a_buf, xt, acc, core_rx, z_rx, xg, own, edge,
    a_sem, in_sem, out_sem, ag_send, ag_recv, relay_send, core_send, core_recv, z_send, z_recv,
):
    n_z, n_x, n_y = plan.n_z, plan.n_x, plan.n_y
    chunk, chunks, width, piece = plan.chunk, plan.chunks, plan.width, plan.piece
    steps = plan.steps
    row, z, core = lax.axis_index("row"), lax.axis_index("col"), lax.axis_index("depth")
    x, y = lax.rem(row, n_x), lax.div(row, n_x)
    at_left, at_right = z == 0, z == n_z - 1

    x_rows = [y * n_x + lax.rem(x + i, n_x) for i in range(1, n_x)]
    y_rows = [lax.rem(y + i, n_y) * n_x + x for i in range(1, n_y)]
    diagonal = [
        lax.rem(y + i, n_y) * n_x + lax.rem(x + k, n_x) for i in range(1, n_y) for k in range(1, n_x)
    ]
    left, right = (row, z - 1, core), (row, z + 1, core)
    partner = (row, z, 1 - core)

    def piece_of(at):
        return sum(jnp.where(at >= n * chunks, 1, 0) for n in range(1, n_z))

    def rightward(q):
        return q + (n_z - 1 - 2 * piece_of(q)) * chunks

    def place_of(at, on_core):
        return at + (piece_of(at) + on_core) * chunks

    def step_ids(k):
        one = jnp.where(at_left, rightward(2 * k), jnp.where(at_right, 2 * k, rightward(k)))
        two = jnp.where(at_left, rightward(2 * k + 1), jnp.where(at_right, 2 * k + 1, k))
        return one, two

    def loads(k, slot):
        if not plan.fused:
            lanes = pl.ds(pl.multiple_of(k * plan.lanes, LANES), plan.lanes)
            return [pltpu.make_async_copy(columns.at[:, 0, :, lanes], a_buf.at[slot], a_sem.at[slot, 0])]
        result = []
        for at in step_ids(k):
            for on_core in range(2):
                i = len(result)
                lanes = pl.ds(pl.multiple_of(place_of(at, on_core) * chunk, LANES), chunk)
                result.append(
                    pltpu.make_async_copy(
                        columns.at[:, 0, :, lanes],
                        a_buf.at[slot, :, :, i * chunk:(i + 1) * chunk],
                        a_sem.at[slot, i],
                    )
                )
        return result

    def load(k, slot):
        for copy in loads(k, slot):
            copy.start(priority=1)

    def ring_step(i):
        i = jnp.where(i >= plan.ringed, i - plan.ringed, i)
        return jnp.where(i <= plan.resident, 2 * i, plan.resident + i)

    def ring_slot(i):
        return plan.resident + lax.rem(i, RING)

    source_in = pltpu.make_async_copy(source, edge.at[0], in_sem)
    source_in.start()
    if plan.ringed == 0:
        for k in range(steps):
            load(k, k)
    else:
        for k in range(max(2 * plan.resident, 2 * RING)):
            if k % 2 == 1 and k < 2 * plan.resident:
                load(k, k // 2)
            if k % 2 == 0 and k < 2 * RING:
                load(ring_step(k // 2), ring_slot(k // 2))

    barrier = pltpu.get_barrier_semaphore()
    for other in x_rows + y_rows:
        pl.semaphore_signal(barrier, inc=1, device_id=(other, z, core), device_id_type=MESH)
    pl.semaphore_signal(barrier, inc=1, device_id=partner, device_id_type=MESH)

    @pl.when(jnp.logical_not(at_left))
    def _():
        pl.semaphore_signal(barrier, inc=1, device_id=left, device_id_type=MESH)

    @pl.when(jnp.logical_not(at_right))
    def _():
        pl.semaphore_signal(barrier, inc=1, device_id=right, device_id_type=MESH)

    beside = jnp.where(at_left, 0, 1) + jnp.where(at_right, 0, 1)

    source_in.wait()
    for j in range(chunks):
        own[0, j] = edge[0, j].T

    pl.semaphore_wait(barrier, n_x + n_y - 1 + beside)

    def spread(p, j, i, other):
        return pltpu.make_async_remote_copy(
            src_ref=own.at[p, j], dst_ref=xg.at[p, row, j],
            send_sem=ag_send.at[p, j, i], recv_sem=ag_recv.at[p, row, j],
            device_id=(other, z, core), device_id_type=MESH,
        )

    def relay(p, j, i, origin, other):
        return pltpu.make_async_remote_copy(
            src_ref=xg.at[p, origin, j], dst_ref=xg.at[p, origin, j],
            send_sem=relay_send.at[p, j, i], recv_sem=ag_recv.at[p, origin, j],
            device_id=(other, z, core), device_id_type=MESH,
        )

    def spread_all(p, j):
        for i, other in enumerate(x_rows + y_rows):
            spread(p, j, i, other).start()

    def pass_on(p, j, near, far):
        for i, origin in enumerate(near):
            relay(p, j, 0, origin, row).wait_recv()
            for k, other in enumerate(far):
                relay(p, j, i * len(far) + k, origin, other).start()

    def place(origin, j, ref):
        high, low = split(ref[...])
        xt[origin, :width, j * chunk:(j + 1) * chunk] = high
        xt[origin, width:, j * chunk:(j + 1) * chunk] = low

    def sides(j):
        return (x_rows, y_rows) if j % 2 == 0 else (y_rows, x_rows)

    def gather(p):
        @pl.when(p == 0)
        def _():
            for j in range(chunks):
                pass_on(p, j, *sides(j))

        for j in range(chunks):
            near, far = sides(j)
            place(row, j, own.at[p, j])
            for origin in near:
                place(origin, j, xg.at[p, origin, j])
            for origin in far:
                relay(p, j, 0, origin, row).wait_recv()
                place(origin, j, xg.at[p, origin, j])
        for j in range(chunks):
            for origin in diagonal:
                relay(p, j, 0, origin, row).wait_recv()
                place(origin, j, xg.at[p, origin, j])

    def to_core(p, at):
        return pltpu.make_async_remote_copy(
            src_ref=acc.at[p, place_of(at, 1 - core)],
            dst_ref=core_rx.at[p, at],
            send_sem=core_send.at[p, at], recv_sem=core_recv.at[p, at],
            device_id=partner, device_id_type=MESH,
        )

    def along(p, at, slot, other):
        return pltpu.make_async_remote_copy(
            src_ref=acc.at[p, place_of(at, core)],
            dst_ref=z_rx.at[p, slot],
            send_sem=z_send.at[p, at], recv_sem=z_recv.at[p, slot],
            device_id=other, device_id_type=MESH,
        )

    def to_right(p, q):
        return along(p, rightward(q), q, right)

    def to_left(p, q):
        return along(p, q, plan.arrivals - 1 - q, left)

    def sent(p, at):
        to_core(p, at).wait_send()

        @pl.when(piece_of(at) != z)
        def _():
            along(p, at, 0, right).wait_send()

    def sent_all(p):
        def one(at, carry):
            sent(p, at)
            return carry

        lax.fori_loop(0, plan.ids, one, 0)

    def multiply(p, k):
        if plan.ringed == 0:
            held, slot = True, k
        else:
            held = jnp.logical_and(lax.rem(k, 2) == 1, k < 2 * plan.resident)
            ring_at = p * plan.ringed + jnp.where(k < 2 * plan.resident, lax.div(k, 2), k - plan.resident)
            slot = jnp.where(held, lax.div(k, 2), ring_slot(ring_at))

        @pl.when(jnp.logical_or(p == 0, jnp.logical_not(held)))
        def _():
            for copy in loads(k, slot):
                copy.wait()

        main = rest = None
        for a in range(plan.outer):
            for at in range(0, piece, plan.k_depth):
                span = slice(at, at + plan.k_depth)
                high, low = split(a_buf[slot, a, span, :])
                both = jnp.dot(xt[a, :, span], high, preferred_element_type=jnp.float32)
                side = jnp.dot(xt[a, :width, span], low, preferred_element_type=jnp.float32)
                main = both if main is None else main + both
                rest = side if rest is None else rest + side
        total = main[:width] + (main[width:] + rest)
        if plan.fused:
            at = [place_of(at, on_core) for at in step_ids(k) for on_core in range(2)]
        else:
            at = [k * plan.per_step + i for i in range(plan.per_step)]
        for i, where in enumerate(at):
            acc[p, where] = total[:, i * chunk:(i + 1) * chunk]

        if plan.ringed > 0:
            follow = ring_at + RING

            @pl.when(jnp.logical_and(jnp.logical_not(held), follow < PASSES * plan.ringed))
            def _():
                load(ring_step(follow), ring_slot(follow))

    def own_sum(p, at):
        to_core(p, at).wait_recv()
        mine = place_of(at, core)
        acc[p, mine] = acc[p, mine] + core_rx[p, at]
        return mine

    def add_from_left(p, q, mine):
        to_right(p, q).wait_recv()
        acc[p, mine] = acc[p, mine] + z_rx[p, q]

    def add_from_right(p, q, mine):
        to_left(p, q).wait_recv()
        acc[p, mine] = acc[p, mine] + z_rx[p, plan.arrivals - 1 - q]

    def finish(p, f):
        mine = own_sum(p, z * chunks + f)

        @pl.when(jnp.logical_not(at_left))
        def _():
            add_from_left(p, (n_z - 1 - z) * chunks + f, mine)

        @pl.when(jnp.logical_not(at_right))
        def _():
            add_from_right(p, z * chunks + f, mine)

        image = acc[p, mine]
        own[p + 1, f] = image
        edge[p, f] = image.T

        @pl.when(p == 0)
        def _():
            spread_all(1, f)
            pltpu.make_async_copy(edge.at[0, f], first.at[f], out_sem.at[0, f]).start()

        @pl.when(p == 1)
        def _():
            pltpu.make_async_copy(edge.at[1, f], second.at[f], out_sem.at[1, f]).start()

    first_final = sum(jnp.where(z == at, plan.final_start(at), 0) for at in range(n_z))

    def iteration(i, p):
        k = i

        @pl.when(k < steps)
        def _():
            multiply(p, k)

            if plan.fused:
                for at in step_ids(k):
                    to_core(p, at).start()
            else:
                @pl.when(k == steps - 1)
                def _():
                    def one(at, inner):
                        to_core(p, at).start()
                        return inner

                    lax.fori_loop(0, plan.ids, one, 0)

        w = i - plan.base - z * LAG + jnp.where(jnp.logical_and(p > 0, z > 0), LAG - 1, 0)
        for u in range(2 if plan.fused else 1):
            q = jnp.where(at_left, 2 * w + u, w) if plan.fused else w
            also = jnp.logical_or(u == 0, at_left)
            inside = jnp.logical_and(w >= 0, q < (n_z - 1 - z) * chunks)

            @pl.when(jnp.logical_and(also, inside))
            def _(q=q):
                mine = own_sum(p, rightward(q))

                @pl.when(jnp.logical_not(at_left))
                def _():
                    add_from_left(p, q, mine)

                to_right(p, q).start()

        w = i - plan.base - (n_z - 1 - z) * LAG + jnp.where(jnp.logical_and(p > 0, z < n_z - 1), LAG - 1, 0)
        for u in range(2 if plan.fused else 1):
            q = jnp.where(at_right, 2 * w + u, w) if plan.fused else w
            also = jnp.logical_or(u == 0, at_right)
            inside = jnp.logical_and(w >= 0, q < z * chunks)

            @pl.when(jnp.logical_and(also, inside))
            def _(q=q):
                mine = own_sum(p, q)

                @pl.when(jnp.logical_not(at_right))
                def _():
                    add_from_right(p, q, mine)

                to_left(p, q).start()

        f = i - first_final

        @pl.when(jnp.logical_and(f >= 0, f < chunks))
        def _():
            finish(p, f)

        j = f - RELAY
        due = jnp.logical_and(p + 1 < PASSES, jnp.logical_and(j >= 0, j < chunks))
        for parity in range(2):
            @pl.when(jnp.logical_and(due, lax.rem(j, 2) == parity))
            def _(parity=parity):
                pass_on(p + 1, j, *sides(parity))

        return p

    for j in range(chunks):
        spread_all(0, j)

    def one_pass(p, carry):
        gather(p)
        lax.fori_loop(0, plan.period, iteration, p)
        return carry

    lax.fori_loop(0, PASSES, one_pass, 0)

    sent_all(0)
    sent_all(1)
    for p in range(PASSES):
        for j in range(chunks):
            for i, other in enumerate(x_rows + y_rows):
                spread(p, j, i, other).wait_send()
            for i in range((n_x - 1) * (n_y - 1)):
                relay(p, j, i, row, row).wait_send()
    for j in range(chunks):
        pltpu.make_async_copy(edge.at[0, j], first.at[j], out_sem.at[0, j]).wait()
        pltpu.make_async_copy(edge.at[1, j], second.at[j], out_sem.at[1, j]).wait()


def hand_over(first_in, second_in, first, second):
    first[...] = first_in[...]
    second[...] = second_in[...]


def solution(mesh):
    def body(matrix_columns, sources):
        plan = Plan(dict(mesh.shape), matrix_columns.shape, sources.shape[-1])
        blocked = (plan.chunks, plan.chunk, plan.width)
        image = jax.ShapeDtypeStruct(blocked, jnp.float32)
        anywhere = pl.BlockSpec(memory_space=pl.ANY)
        products = 2 * plan.rows * plan.outer * plan.piece
        first, second = pl.pallas_call(
            functools.partial(chain_kernel, plan),
            out_shape=(image, image),
            in_specs=[anywhere, anywhere],
            out_specs=(anywhere, anywhere),
            scratch_shapes=plan.scratch(),
            compiler_params=pltpu.CompilerParams(
                collective_id=0, has_side_effects=True, vmem_limit_bytes=VMEM_BYTES
            ),
            cost_estimate=pl.CostEstimate(
                flops=6 * products * plan.width, bytes_accessed=4 * products, transcendentals=0
            ),
        )(matrix_columns, sources.reshape(blocked))
        first, second = pl.pallas_call(
            hand_over,
            out_shape=(image, image),
            in_specs=[pl.BlockSpec(memory_space=pltpu.VMEM)] * 2,
            out_specs=(pl.BlockSpec(memory_space=pltpu.VMEM),) * 2,
        )(first, second)
        return first.reshape(sources.shape), second.reshape(sources.shape)

    in_specs = (P(None, ("col", "depth"), None, "row"), P("row", ("col", "depth"), None, None))
    out_specs = (P("row", ("col", "depth"), None, None), P("row", ("col", "depth"), None, None))
    return jax.shard_map(body, mesh=mesh, in_specs=in_specs, out_specs=out_specs, check_vma=False)
```
